32 devices in a mesh: pairs: 2 (over y), aa: 4 (over z), ba: 4 (over x, core).
Axes of the slice: x: 2, y: 2, z: 4, core: 2. Of those that a mesh axis runs over, the one named last changes fastest.
Arguments:
- feats_a: float32 [1024, 256], P(('pairs', 'aa', 'ba')), parts along dimension 0, may hold values from -24 to 24
- feats_b: float32 [512, 256], P(('pairs', 'ba', 'aa')), parts along dimension 0, may hold values from -24 to 24
- qk_weight: float32 [2, 256, 256], replicated, may hold values from -0.375 to 0.375
- qk_bias: float32 [2, 256], replicated, may hold values from -3 to 3
- value_weight: float32 [2, 256, 256], replicated, may hold values from -0.375 to 0.375
- value_bias: float32 [2, 256], replicated, may hold values from -3 to 3
- out_weight: float32 [2, 256, 256], replicated, may hold values from -0.375 to 0.375
- out_bias: float32 [2, 256], replicated, may hold values from -3 to 3
- hidden_weight: float32 [2, 512, 512], replicated, may hold values from -0.25 to 0.25
- hidden_bias: float32 [2, 512], replicated, may hold values from -3 to 3
- norm_gain: float32 [2, 512], replicated, may hold values from 0.25 to 1.75
- norm_bias: float32 [2, 512], replicated, may hold values from -3 to 3
- final_weight: float32 [2, 512, 256], replicated, may hold values from -0.25 to 0.25
- final_bias: float32 [2, 256], replicated, may hold values from -3 to 3
Outputs:
- out_a: float32 [1024, 256], P(('pairs', 'aa', 'ba')), parts along dimension 0
- out_b: float32 [512, 256], P(('pairs', 'ba', 'aa')), parts along dimension 0
The draws below stay inside these ranges and needn't reach their ends.
There are 2 independent parts, one for each index of `pairs`. The reference program is written for one: setup_inputs(seed, part) draws one part's arguments, and reference() takes and returns one part's arrays. A program takes and returns all parts, laid end to end along the dimension named above; an argument that names none is the same for every part. Nothing has to cross between parts.
All inputs are finite; a program needn't handle non-finite values.
Results may differ from the reference program's by a relative error of at most 0.0003.
Values sent between devices are 32-bit elements; how exact they have to be, the bound alone decides.
A program may use at most 64 MiB of HBM per device.

```python
import math
import jax
import jax.numpy as jnp
from jax import lax

D = 256
HEADS = 4
HEAD_SIZE = 64
WIDE = 512
LAYERS = 2
M = 512
N = 256


def draw_features(key, row_count, salt_value):
    values = jnp.clip(jax.random.normal(jax.random.fold_in(key, salt_value), (row_count, D), jnp.float32), -6.0, 6.0)
    return values


def draw_feats_a(key, part):
    return draw_features(key, M, 11)


def draw_feats_b(key, part):
    return draw_features(key, N, 31)


def scatter_about(rng, shape, scale, limit, held_as=jnp.bfloat16):
    entries = jax.random.normal(rng, shape, jnp.float32) * scale
    return jnp.minimum(jnp.maximum(entries, -limit), limit).astype(held_as)


def setup_inputs(seed: int = 0, part: int = 0) -> dict:
    arg_keys = jax.random.split(jax.random.key(seed), 15)
    own_keys = jax.random.split(jax.random.fold_in(arg_keys[14], part), 15)
    return {
        "feats_a": draw_feats_a(jax.random.fold_in(jax.random.fold_in(arg_keys[14], part), 71), part),
        "feats_b": draw_feats_b(jax.random.fold_in(jax.random.fold_in(arg_keys[14], part), 71), part),
        "qk_weight": scatter_about(arg_keys[2], (LAYERS, D, D), D ** -0.5, 0.375, jnp.float32),
        "qk_bias": scatter_about(arg_keys[3], (LAYERS, D), 0.5, 3.0, jnp.float32),
        "value_weight": scatter_about(arg_keys[4], (LAYERS, D, D), D ** -0.5, 0.375, jnp.float32),
        "value_bias": scatter_about(arg_keys[5], (LAYERS, D), 0.5, 3.0, jnp.float32),
        "out_weight": scatter_about(arg_keys[6], (LAYERS, D, D), D ** -0.5, 0.375, jnp.float32),
        "out_bias": scatter_about(arg_keys[7], (LAYERS, D), 0.5, 3.0, jnp.float32),
        "hidden_weight": scatter_about(arg_keys[8], (LAYERS, WIDE, WIDE), WIDE ** -0.5, 0.25, jnp.float32),
        "hidden_bias": scatter_about(arg_keys[9], (LAYERS, WIDE), 0.5, 3.0, jnp.float32),
        "norm_gain": jnp.clip(1.0 + 0.15 * jax.random.normal(arg_keys[10], (LAYERS, WIDE), jnp.float32), 0.25, 1.75),
        "norm_bias": scatter_about(arg_keys[11], (LAYERS, WIDE), 0.5, 3.0, jnp.float32),
        "final_weight": scatter_about(arg_keys[12], (LAYERS, WIDE, D), WIDE ** -0.5, 0.25, jnp.float32),
        "final_bias": scatter_about(arg_keys[13], (LAYERS, D), 0.5, 3.0, jnp.float32),
    }


EXACT_RESULT = lax.Precision.HIGHEST

def matmul(left, right):
    return jnp.dot(left, right, precision=EXACT_RESULT)

def layer_norm(values, gain, offset):
    average = lax.optimization_barrier(jnp.mean(values, -1, keepdims=True))
    centred = values - average
    spread = lax.optimization_barrier(jnp.mean(centred * centred, -1, keepdims=True))
    return centred / jnp.sqrt(spread + 1e-05) * gain + offset

def feed_forward(state, message, hidden_weight, hidden_bias, norm_gain, norm_bias, final_weight, final_bias):
    joined = jnp.concatenate([state, message], -1)
    hidden = matmul(joined, hidden_weight) + hidden_bias
    active = jax.nn.gelu(layer_norm(hidden, norm_gain, norm_bias), approximate=False)
    return state + matmul(active, final_weight) + final_bias

def cross_messages(query_first_image, value_a, query_second_image, value_b):
    block_rows = math.gcd(M, 1024)
    count = M // block_rows
    softmax_temper = HEAD_SIZE ** (-0.5)
    query_blocks = query_first_image.reshape(count, block_rows, HEADS, HEAD_SIZE)
    value_blocks = value_a.reshape(count, block_rows, HEADS, HEAD_SIZE)

    def advance(running, pieces):
        col_top, col_sum, numerator = running
        query_slice, value_piece = pieces
        score_matrix = jnp.einsum('cjg,xjg->jcx', query_slice, query_second_image, precision=EXACT_RESULT) * softmax_temper
        row_top = lax.optimization_barrier(jnp.max(score_matrix, 2, keepdims=True))
        row_exp = jnp.exp(score_matrix - row_top)
        row_sum = jnp.transpose(lax.optimization_barrier(jnp.sum(row_exp, 2)))
        row_msg = jnp.einsum('hab,bhd->ahd', row_exp, value_b, precision=EXACT_RESULT) / row_sum[:, :, None]
        new_top = jnp.maximum(col_top, lax.optimization_barrier(jnp.max(score_matrix, 1)))
        col_exp = jnp.exp(score_matrix - new_top[:, None, :])
        rescale = jnp.exp(col_top - new_top)
        col_sum = col_sum * rescale + lax.optimization_barrier(jnp.sum(col_exp, 1))
        numerator = numerator * rescale[:, :, None] + jnp.einsum('hab,ahd->hbd', col_exp, value_piece, precision=EXACT_RESULT)
        return ((new_top, col_sum, numerator), row_msg)
    start = (jnp.full((HEADS, N), -jnp.inf, jnp.float32), jnp.zeros((HEADS, N), jnp.float32), jnp.zeros((HEADS, N, HEAD_SIZE), jnp.float32))
    running, row_blocks = lax.scan(advance, start, (query_blocks, value_blocks))
    msg_a = row_blocks.reshape(M, D)
    msg_b = jnp.transpose(running[2] / running[1][:, :, None], (1, 0, 2)).reshape(N, D)
    return (msg_a, msg_b)

def reference(feats_a, feats_b, qk_weight, qk_bias, value_weight, value_bias, out_weight, out_bias, hidden_weight, hidden_bias, norm_gain, norm_bias, final_weight, final_bias):
    first = feats_a
    second = feats_b
    for layer_index in range(LAYERS):
        query_first_image = (matmul(first, qk_weight[layer_index]) + qk_bias[layer_index]).reshape(M, HEADS, HEAD_SIZE)
        value_a = (matmul(first, value_weight[layer_index]) + value_bias[layer_index]).reshape(M, HEADS, HEAD_SIZE)
        query_second_image = (matmul(second, qk_weight[layer_index]) + qk_bias[layer_index]).reshape(N, HEADS, HEAD_SIZE)
        value_b = (matmul(second, value_weight[layer_index]) + value_bias[layer_index]).reshape(N, HEADS, HEAD_SIZE)
        msg_a, msg_b = cross_messages(query_first_image, value_a, query_second_image, value_b)
        reply_a = matmul(msg_a, out_weight[layer_index]) + out_bias[layer_index]
        reply_b = matmul(msg_b, out_weight[layer_index]) + out_bias[layer_index]
        first = feed_forward(first, reply_a, hidden_weight[layer_index], hidden_bias[layer_index], norm_gain[layer_index], norm_bias[layer_index], final_weight[layer_index], final_bias[layer_index])
        second = feed_forward(second, reply_b, hidden_weight[layer_index], hidden_bias[layer_index], norm_gain[layer_index], norm_bias[layer_index], final_weight[layer_index], final_bias[layer_index])
    return (first, second)
```

```python
import functools

import jax
import jax.numpy as jnp
from jax import lax
from jax.experimental import pallas as pl
from jax.experimental.pallas import tpu as pltpu
from jax.sharding import PartitionSpec as P

HEADS = 4
LANES = 128
F32 = jnp.float32
BF16 = jnp.bfloat16
NN = (((1,), (0,)), ((), ()))
NT = (((1,), (1,)), ((), ()))


def split(x):
    hi = x.astype(BF16)
    return hi, (x - hi.astype(F32)).astype(BF16)


def dot3(a, b, dims=NN):
    f = functools.partial(lax.dot_general, dimension_numbers=dims, preferred_element_type=F32)
    return f(a[0], b[0]) + (f(a[1], b[0]) + f(a[0], b[1]))


def erf(x):
    x = jnp.clip(x, -3.832506856900711, 3.832506856900711)
    z = x * x
    p = jnp.full_like(z, 0.00022905065861350646)
    for c in (0.0034082910107109506, 0.050955695062380861, 0.18520832239976145, 1.128379143519084):
        p = p * z + c
    q = jnp.full_like(z, -1.1791602954361697e-7)
    for c in (
        0.000023547966471313185,
        0.0010179625278914885,
        0.014070470171167667,
        0.11098505178285362,
        0.49746925110067538,
        1.0,
    ):
        q = q * z + c
    return x * p / q


def head_masks(width):
    lane = lax.broadcasted_iota(jnp.int32, (1, width), 1)
    size = width // HEADS
    return [(lane >= h * size) & (lane < (h + 1) * size) for h in range(HEADS)]


def attend(q, k, v, scale):
    width = q[0].shape[1]
    cols = k[0].shape[0]
    ones = [m.astype(F32).astype(BF16) for m in head_masks(width)]
    kb = [jnp.concatenate([part * m for m in ones], 0) for part in k]
    vb = [jnp.concatenate([part * m for m in ones], 0) for part in v]
    s = dot3(q, kb, NT) * scale
    lane = lax.broadcasted_iota(jnp.int32, (1, LANES), 1)
    stats = jnp.zeros((s.shape[0], LANES), F32)
    if cols % LANES == 0:
        parts = []
        for h in range(HEADS):
            sh = s[:, h * cols : (h + 1) * cols]
            top = jnp.max(sh, 1, keepdims=True)
            e = jnp.exp(sh - top)
            total = jnp.sum(e, 1, keepdims=True)
            parts.append(e)
            stats = jnp.where(lane == h, top, jnp.where(lane == HEADS + h, total, stats))
        e = jnp.concatenate(parts, 1)
    else:
        masks = head_masks(s.shape[1])
        shift = jnp.zeros_like(s)
        for h in range(HEADS):
            top = jnp.max(jnp.where(masks[h], s, -jnp.inf), 1, keepdims=True)
            shift = jnp.where(masks[h], top, shift)
            stats = jnp.where(lane == h, top, stats)
        e = jnp.exp(s - shift)
        for h in range(HEADS):
            total = jnp.sum(jnp.where(masks[h], e, 0.0), 1, keepdims=True)
            stats = jnp.where(lane == HEADS + h, total, stats)
    return dot3(split(e), vb), stats


def settle(got, layer):
    sources, rows, packed = got.shape[1:]
    width = packed - LANES
    masks = head_masks(width)
    stats = [got[layer, i, :, width:] for i in range(sources)]
    best = functools.reduce(jnp.maximum, stats)
    weights = [jnp.exp(st - best) for st in stats]
    denom = sum(w * pltpu.roll(st, LANES - HEADS, 1) for w, st in zip(weights, stats))
    out = jnp.zeros((rows, width), F32)
    for i in range(sources):
        c = weights[i] / denom
        full = jnp.zeros((rows, width), F32)
        for h in range(HEADS):
            full = jnp.where(masks[h], c[:, h : h + 1], full)
        out = out + full * got[layer, i, :, :width]
    return out


def kernel(na, nb, *refs):
    (fa, fb), weights, (out_a, out_b) = refs[:2], refs[2:14], refs[14:16]
    (xa, xb, sa, sb, ga, gb), rest = refs[16:22], refs[22:]
    held, rest = rest[:12], rest[12:]
    his, los = rest[:5], rest[5:10]
    load, in_sem, xs, xr, ys, yr, ps, pr, qs, qr = rest[10:]
    wqk, bqk, wv, bv, wo, bo, wh, bh, gain, nbias, wf, bf = held
    layers, _, ra, width = xa.shape
    rb = xb.shape[2]
    scale = (width // HEADS) ** (-0.5)
    ma, mb = lax.axis_index("ba"), lax.axis_index("aa")

    first = [
        pltpu.make_async_copy(fa, xa.at[0, ma], in_sem.at[0]),
        pltpu.make_async_copy(fb, xb.at[0, mb], in_sem.at[1]),
    ]
    for c in first:
        c.start()
    loads = [pltpu.make_async_copy(w, h, load.at[i]) for i, (w, h) in enumerate(zip(weights, held))]
    for c in loads:
        c.start()

    barrier = pltpu.get_barrier_semaphore()
    for axis, me, n in (("ba", ma, nb), ("aa", mb, na)):
        for d in range(1, n):
            pl.semaphore_signal(
                barrier,
                inc=1,
                device_id={axis: (me + d) % n},
                device_id_type=pl.DeviceIdType.MESH,
            )
    pl.semaphore_wait(barrier, na + nb - 2)
    for c in first:
        c.wait()

    sent = []

    def exchange(axis, me, n, source, target, layer, ssem, rsem):
        arrive = []
        for d in range(1, n):
            peer = (me + d) % n
            copy = pltpu.make_async_remote_copy(
                src_ref=source(peer),
                dst_ref=target.at[layer, me],
                send_sem=ssem.at[layer, d],
                recv_sem=rsem.at[layer, me],
                device_id={axis: peer},
                device_id_type=pl.DeviceIdType.MESH,
            )
            copy.start()
            sent.append(copy)
            arrive.append(
                pltpu.make_async_remote_copy(
                    src_ref=target.at[layer, peer],
                    dst_ref=target.at[layer, peer],
                    send_sem=ssem.at[layer, d],
                    recv_sem=rsem.at[layer, peer],
                    device_id={axis: peer},
                    device_id_type=pl.DeviceIdType.MESH,
                )
            )
        return arrive

    matrices = (wqk, wv, wo, wh, wf)

    def narrow(which, layer):
        for i in which:
            his[i][layer], los[i][layer] = split(matrices[i][layer])

    def wide(i, layer):
        return his[i][layer], los[i][layer]

    for l in range(layers):
        arrive = exchange("aa", mb, na, lambda p: xb.at[l, mb], xb, l, ys, yr)
        arrive += exchange("ba", ma, nb, lambda p: xa.at[l, ma], xa, l, xs, xr)
        if l == 0:
            for c in loads:
                c.wait()
            narrow(range(5), 0)
        for c in arrive:
            c.wait_recv()
        rows_a = split(xa[l].reshape(nb * ra, width))
        rows_b = split(xb[l].reshape(na * rb, width))
        w, u = wide(0, l), wide(1, l)
        qa = split(dot3(rows_a, w) + bqk[l : l + 1])
        va = split(dot3(rows_a, u) + bv[l : l + 1])
        qb = split(dot3(rows_b, w) + bqk[l : l + 1])
        vb = split(dot3(rows_b, u) + bv[l : l + 1])

        numer, stats = attend(qb, qa, va, scale)
        sb[l, :, :, :width] = numer.reshape(na, rb, width)
        sb[l, :, :, width:] = stats.reshape(na, rb, LANES)
        arrive = exchange("aa", mb, na, lambda p: sb.at[l, p], gb, l, qs, qr)
        numer, stats = attend(qa, qb, vb, scale)
        sa[l, :, :, :width] = numer.reshape(nb, ra, width)
        sa[l, :, :, width:] = stats.reshape(nb, ra, LANES)
        arrive += exchange("ba", ma, nb, lambda p: sa.at[l, p], ga, l, ps, pr)
        ga[l, ma] = sa[l, ma]
        gb[l, mb] = sb[l, mb]
        if l + 1 < layers:
            narrow(range(5), l + 1)
        for c in arrive:
            c.wait_recv()

        x = jnp.concatenate([xa[l, ma], xb[l, mb]], 0)
        msg = jnp.concatenate([settle(ga, l), settle(gb, l)], 0)
        y = dot3(split(msg), wide(2, l)) + bo[l : l + 1]
        joined = split(jnp.concatenate([x, y], 1))
        hidden = dot3(joined, wide(3, l)) + bh[l : l + 1]
        centred = hidden - jnp.mean(hidden, 1, keepdims=True)
        spread = jnp.mean(centred * centred, 1, keepdims=True)
        normed = centred / jnp.sqrt(spread + 1e-05) * gain[l : l + 1] + nbias[l : l + 1]
        active = 0.5 * normed * (1.0 + erf(normed * (0.5**0.5)))
        x = x + dot3(split(active), wide(4, l)) + bf[l : l + 1]
        if l + 1 < layers:
            xa[l + 1, ma] = x[:ra]
            xb[l + 1, mb] = x[ra:]
        else:
            out_a[...] = x[:ra]
            out_b[...] = x[ra:]
    for c in sent:
        c.wait_send()


def shards(na, nb, *args):
    fa, fb, *weights = args
    layers = weights[0].shape[0]
    (ra, width), rb = fa.shape, fb.shape[0]
    packed = width + LANES
    matrices = [weights[i] for i in (0, 2, 4, 6, 10)]
    dma = pltpu.SemaphoreType.DMA
    scratch = [
        pltpu.VMEM((layers, nb, ra, width), F32),
        pltpu.VMEM((layers, na, rb, width), F32),
        pltpu.VMEM((layers, nb, ra, packed), F32),
        pltpu.VMEM((layers, na, rb, packed), F32),
        pltpu.VMEM((layers, nb, ra, packed), F32),
        pltpu.VMEM((layers, na, rb, packed), F32),
    ]
    scratch += [pltpu.VMEM(w.shape, F32) for w in weights]
    scratch += [pltpu.VMEM(w.shape, BF16) for w in matrices] * 2
    scratch += [dma((len(weights),)), dma((2,))]
    scratch += [dma((layers, n)) for n in (nb, nb, na, na, nb, nb, na, na)]
    any_spec = pl.BlockSpec(memory_space=pl.ANY)
    vmem = pl.BlockSpec(memory_space=pltpu.VMEM)
    return tuple(
        pl.pallas_call(
            functools.partial(kernel, na, nb),
            out_shape=(
                jax.ShapeDtypeStruct(fa.shape, F32),
                jax.ShapeDtypeStruct(fb.shape, F32),
            ),
            in_specs=[any_spec] * len(args),
            out_specs=(vmem, vmem),
            scratch_shapes=scratch,
            compiler_params=pltpu.CompilerParams(
                collective_id=0, has_side_effects=True, vmem_limit_bytes=60 * 1024 * 1024
            ),
        )(*args)
    )


def solution(mesh):
    in_specs = (P(("pairs", "aa", "ba"), None), P(("pairs", "ba", "aa"), None)) + (P(),) * 12
    out_specs = (P(("pairs", "aa", "ba"), None), P(("pairs", "ba", "aa"), None))
    return jax.shard_map(
        functools.partial(shards, mesh.shape["aa"], mesh.shape["ba"]),
        mesh=mesh,
        in_specs=in_specs,
        out_specs=out_specs,
        check_vma=False,
    )
```

```python
import functools

import jax
import jax.numpy as jnp
from jax import lax
from jax.experimental import pallas as pl
from jax.experimental.pallas import tpu as pltpu
from jax.sharding import PartitionSpec as P

HEADS = 4
LANES = 128
F32 = jnp.float32
BF16 = jnp.bfloat16
NN = (((1,), (0,)), ((), ()))
NT = (((1,), (1,)), ((), ()))


def split(x):
    hi = x.astype(BF16)
    return hi, (x - hi.astype(F32)).astype(BF16)


def dot3(a, b, dims=NN):
    f = functools.partial(lax.dot_general, dimension_numbers=dims, preferred_element_type=F32)
    return f(a[0], b[0]) + (f(a[1], b[0]) + f(a[0], b[1]))


def erf(x):
    x = jnp.clip(x, -3.832506856900711, 3.832506856900711)
    z = x * x
    p = jnp.full_like(z, 0.00022905065861350646)
    for c in (0.0034082910107109506, 0.050955695062380861, 0.18520832239976145, 1.128379143519084):
        p = p * z + c
    q = jnp.full_like(z, -1.1791602954361697e-7)
    for c in (
        0.000023547966471313185,
        0.0010179625278914885,
        0.014070470171167667,
        0.11098505178285362,
        0.49746925110067538,
        1.0,
    ):
        q = q * z + c
    return x * p / q


def head_masks(width):
    lane = lax.broadcasted_iota(jnp.int32, (1, width), 1)
    size = width // HEADS
    return [(lane >= h * size) & (lane < (h + 1) * size) for h in range(HEADS)]


def attend(q, k, v, scale):
    width = q[0].shape[1]
    cols = k[0].shape[0]
    ones = [m.astype(F32).astype(BF16) for m in head_masks(width)]
    kb = [jnp.concatenate([part * m for m in ones], 0) for part in k]
    vb = [jnp.concatenate([part * m for m in ones], 0) for part in v]
    s = dot3(q, kb, NT) * scale
    lane = lax.broadcasted_iota(jnp.int32, (1, LANES), 1)
    stats = jnp.zeros((s.shape[0], LANES), F32)
    if cols % LANES == 0:
        parts = []
        for h in range(HEADS):
            sh = s[:, h * cols : (h + 1) * cols]
            top = jnp.max(sh, 1, keepdims=True)
            e = jnp.exp(sh - top)
            total = jnp.sum(e, 1, keepdims=True)
            parts.append(e)
            stats = jnp.where(lane == h, top, jnp.where(lane == HEADS + h, total, stats))
        e = jnp.concatenate(parts, 1)
    else:
        masks = head_masks(s.shape[1])
        shift = jnp.zeros_like(s)
        for h in range(HEADS):
            top = jnp.max(jnp.where(masks[h], s, -jnp.inf), 1, keepdims=True)
            shift = jnp.where(masks[h], top, shift)
            stats = jnp.where(lane == h, top, stats)
        e = jnp.exp(s - shift)
        for h in range(HEADS):
            total = jnp.sum(jnp.where(masks[h], e, 0.0), 1, keepdims=True)
            stats = jnp.where(lane == HEADS + h, total, stats)
    return dot3(split(e), vb), stats


def settle(got, layer):
    sources, rows, packed = got.shape[1:]
    width = packed - LANES
    masks = head_masks(width)
    stats = [got[layer, i, :, width:] for i in range(sources)]
    best = functools.reduce(jnp.maximum, stats)
    weights = [jnp.exp(st - best) for st in stats]
    denom = sum(w * pltpu.roll(st, LANES - HEADS, 1) for w, st in zip(weights, stats))
    out = jnp.zeros((rows, width), F32)
    for i in range(sources):
        c = weights[i] / denom
        full = jnp.zeros((rows, width), F32)
        for h in range(HEADS):
            full = jnp.where(masks[h], c[:, h : h + 1], full)
        out = out + full * got[layer, i, :, :width]
    return out


def kernel(na, nb, *refs):
    (fa, fb), weights, (out_a, out_b) = refs[:2], refs[2:14], refs[14:16]
    (xa, xb, sa, sb, ga, gb), rest = refs[16:22], refs[22:]
    held, rest = rest[:12], rest[12:]
    his, los = rest[:5], rest[5:10]
    load, vec, in_sem, xs, xr, ys, yr, ps, pr, qs, qr = rest[10:]
    wqk, bqk, wv, bv, wo, bo, wh, bh, gain, nbias, wf, bf = held
    layers, _, ra, width = xa.shape
    rb = xb.shape[2]
    scale = (width // HEADS) ** (-0.5)
    ma, mb = lax.axis_index("ba"), lax.axis_index("aa")

    first = [
        pltpu.make_async_copy(fa, xa.at[0, ma], in_sem.at[0]),
        pltpu.make_async_copy(fb, xb.at[0, mb], in_sem.at[1]),
    ]
    for c in first:
        c.start()
    small = [(w, h) for w, h in zip(weights, held) if len(w.shape) == 2]
    large = [(w, h) for w, h in zip(weights, held) if len(w.shape) == 3]
    vectors = [pltpu.make_async_copy(w, h, vec.at[i]) for i, (w, h) in enumerate(small)]
    loads = [
        [pltpu.make_async_copy(w.at[j], h.at[j], load.at[j, i]) for i, (w, h) in enumerate(large)]
        for j in range(layers)
    ]
    for c in loads[0][:2] + vectors + loads[0][2:]:
        c.start()
    for later in loads[1:]:
        for c in later:
            c.start()

    barrier = pltpu.get_barrier_semaphore()
    for axis, me, n in (("ba", ma, nb), ("aa", mb, na)):
        for d in range(1, n):
            pl.semaphore_signal(
                barrier,
                inc=1,
                device_id={axis: (me + d) % n},
                device_id_type=pl.DeviceIdType.MESH,
            )
    pl.semaphore_wait(barrier, na + nb - 2)
    for c in first:
        c.wait()

    sent = []

    def exchange(axis, me, n, source, target, layer, ssem, rsem):
        arrive = []
        for d in range(1, n):
            peer = (me + d) % n
            copy = pltpu.make_async_remote_copy(
                src_ref=source(peer),
                dst_ref=target.at[layer, me],
                send_sem=ssem.at[layer, d],
                recv_sem=rsem.at[layer, me],
                device_id={axis: peer},
                device_id_type=pl.DeviceIdType.MESH,
            )
            copy.start()
            sent.append(copy)
            arrive.append(
                pltpu.make_async_remote_copy(
                    src_ref=target.at[layer, peer],
                    dst_ref=target.at[layer, peer],
                    send_sem=ssem.at[layer, d],
                    recv_sem=rsem.at[layer, peer],
                    device_id={axis: peer},
                    device_id_type=pl.DeviceIdType.MESH,
                )
            )
        return arrive

    matrices = (wqk, wv, wo, wh, wf)

    def narrow(which, layer):
        for i in which:
            loads[layer][i].wait()
            his[i][layer], los[i][layer] = split(matrices[i][layer])

    def wide(i, layer):
        return his[i][layer], los[i][layer]

    for l in range(layers):
        far = exchange("aa", mb, na, lambda p: xb.at[l, mb], xb, l, ys, yr)
        near = exchange("ba", ma, nb, lambda p: xa.at[l, ma], xa, l, xs, xr)
        if l == 0:
            narrow(range(2), 0)
            for c in vectors:
                c.wait()
        for c in near:
            c.wait_recv()
        rows_a = split(xa[l].reshape(nb * ra, width))
        w, u = wide(0, l), wide(1, l)
        qa = split(dot3(rows_a, w) + bqk[l : l + 1])
        va = split(dot3(rows_a, u) + bv[l : l + 1])
        for c in far:
            c.wait_recv()
        rows_b = split(xb[l].reshape(na * rb, width))
        qb = split(dot3(rows_b, w) + bqk[l : l + 1])
        vb = split(dot3(rows_b, u) + bv[l : l + 1])

        numer, stats = attend(qb, qa, va, scale)
        sb[l, :, :, :width] = numer.reshape(na, rb, width)
        sb[l, :, :, width:] = stats.reshape(na, rb, LANES)
        arrive = exchange("aa", mb, na, lambda p: sb.at[l, p], gb, l, qs, qr)
        numer, stats = attend(qa, qb, vb, scale)
        sa[l, :, :, :width] = numer.reshape(nb, ra, width)
        sa[l, :, :, width:] = stats.reshape(nb, ra, LANES)
        arrive += exchange("ba", ma, nb, lambda p: sa.at[l, p], ga, l, ps, pr)
        ga[l, ma] = sa[l, ma]
        gb[l, mb] = sb[l, mb]
        if l == 0:
            narrow(range(2, 5), 0)
            for j in range(1, layers):
                narrow(range(5), j)
        for c in arrive:
            c.wait_recv()

        x = jnp.concatenate([xa[l, ma], xb[l, mb]], 0)
        msg = jnp.concatenate([settle(ga, l), settle(gb, l)], 0)
        y = dot3(split(msg), wide(2, l)) + bo[l : l + 1]
        joined = split(jnp.concatenate([x, y], 1))
        hidden = dot3(joined, wide(3, l)) + bh[l : l + 1]
        centred = hidden - jnp.mean(hidden, 1, keepdims=True)
        spread = jnp.mean(centred * centred, 1, keepdims=True)
        normed = centred / jnp.sqrt(spread + 1e-05) * gain[l : l + 1] + nbias[l : l + 1]
        active = 0.5 * normed * (1.0 + erf(normed * (0.5**0.5)))
        x = x + dot3(split(active), wide(4, l)) + bf[l : l + 1]
        if l + 1 < layers:
            xa[l + 1, ma] = x[:ra]
            xb[l + 1, mb] = x[ra:]
        else:
            out_a[...] = x[:ra]
            out_b[...] = x[ra:]
    for c in sent:
        c.wait_send()


def shards(na, nb, *args):
    fa, fb, *weights = args
    layers = weights[0].shape[0]
    (ra, width), rb = fa.shape, fb.shape[0]
    packed = width + LANES
    matrices = [weights[i] for i in (0, 2, 4, 6, 10)]
    dma = pltpu.SemaphoreType.DMA
    scratch = [
        pltpu.VMEM((layers, nb, ra, width), F32),
        pltpu.VMEM((layers, na, rb, width), F32),
        pltpu.VMEM((layers, nb, ra, packed), F32),
        pltpu.VMEM((layers, na, rb, packed), F32),
        pltpu.VMEM((layers, nb, ra, packed), F32),
        pltpu.VMEM((layers, na, rb, packed), F32),
    ]
    scratch += [pltpu.VMEM(w.shape, F32) for w in weights]
    scratch += [pltpu.VMEM(w.shape, BF16) for w in matrices] * 2
    scratch += [dma((layers, len(matrices))), dma((len(weights) - len(matrices),)), dma((2,))]
    scratch += [dma((layers, n)) for n in (nb, nb, na, na, nb, nb, na, na)]
    any_spec = pl.BlockSpec(memory_space=pltpu.HBM)
    vmem = pl.BlockSpec(memory_space=pltpu.VMEM)
    return tuple(
        pl.pallas_call(
            functools.partial(kernel, na, nb),
            out_shape=(
                pltpu.VMEM(fa.shape, F32),
                pltpu.VMEM(fb.shape, F32),
            ),
            in_specs=[any_spec] * len(args),
            out_specs=(vmem, vmem),
            scratch_shapes=scratch,
            compiler_params=pltpu.CompilerParams(
                collective_id=0, has_side_effects=True, vmem_limit_bytes=60 * 1024 * 1024
            ),
        )(*args)
    )


def solution(mesh):
    in_specs = (P(("pairs", "aa", "ba"), None), P(("pairs", "ba", "aa"), None)) + (P(),) * 12
    out_specs = (P(("pairs", "aa", "ba"), None), P(("pairs", "ba", "aa"), None))
    return jax.shard_map(
        functools.partial(shards, mesh.shape["aa"], mesh.shape["ba"]),
        mesh=mesh,
        in_specs=in_specs,
        out_specs=out_specs,
        check_vma=False,
    )
```

```python
import functools

import jax
import jax.numpy as jnp
from jax import lax
from jax.experimental import pallas as pl
from jax.experimental.pallas import tpu as pltpu
from jax.sharding import PartitionSpec as P

HEADS = 4
LANES = 128
F32 = jnp.float32
BF16 = jnp.bfloat16
NN = (((1,), (0,)), ((), ()))
NT = (((1,), (1,)), ((), ()))


def split(x):
    hi = x.astype(BF16)
    return hi, (x - hi.astype(F32)).astype(BF16)


def dot3(a, b, dims=NN):
    f = functools.partial(lax.dot_general, dimension_numbers=dims, preferred_element_type=F32)
    return f(a[0], b[0]) + (f(a[1], b[0]) + f(a[0], b[1]))


def erf(x):
    x = jnp.clip(x, -3.832506856900711, 3.832506856900711)
    z = x * x
    p = jnp.full_like(z, 0.00022905065861350646)
    for c in (0.0034082910107109506, 0.050955695062380861, 0.18520832239976145, 1.128379143519084):
        p = p * z + c
    q = jnp.full_like(z, -1.1791602954361697e-7)
    for c in (
        0.000023547966471313185,
        0.0010179625278914885,
        0.014070470171167667,
        0.11098505178285362,
        0.49746925110067538,
        1.0,
    ):
        q = q * z + c
    return x * p / q


def head_masks(width):
    lane = lax.broadcasted_iota(jnp.int32, (1, width), 1)
    size = width // HEADS
    return [(lane >= h * size) & (lane < (h + 1) * size) for h in range(HEADS)]


def attend(q, k, v, scale):
    width = q[0].shape[1]
    cols = k[0].shape[0]
    ones = [m.astype(F32).astype(BF16) for m in head_masks(width)]
    kb = [jnp.concatenate([part * m for m in ones], 0) for part in k]
    vb = [jnp.concatenate([part * m for m in ones], 0) for part in v]
    s = dot3(q, kb, NT) * scale
    lane = lax.broadcasted_iota(jnp.int32, (1, LANES), 1)
    stats = jnp.zeros((s.shape[0], LANES), F32)
    if cols % LANES == 0:
        parts = []
        for h in range(HEADS):
            sh = s[:, h * cols : (h + 1) * cols]
            top = jnp.max(sh, 1, keepdims=True)
            e = jnp.exp(sh - top)
            total = jnp.sum(e, 1, keepdims=True)
            parts.append(e)
            stats = jnp.where(lane == h, top, jnp.where(lane == HEADS + h, total, stats))
        e = jnp.concatenate(parts, 1)
    else:
        masks = head_masks(s.shape[1])
        shift = jnp.zeros_like(s)
        for h in range(HEADS):
            top = jnp.max(jnp.where(masks[h], s, -jnp.inf), 1, keepdims=True)
            shift = jnp.where(masks[h], top, shift)
            stats = jnp.where(lane == h, top, stats)
        e = jnp.exp(s - shift)
        for h in range(HEADS):
            total = jnp.sum(jnp.where(masks[h], e, 0.0), 1, keepdims=True)
            stats = jnp.where(lane == HEADS + h, total, stats)
    return dot3(split(e), vb), stats


def settle(got, layer):
    sources, rows, packed = got.shape[1:]
    width = packed - LANES
    masks = head_masks(width)
    stats = [got[layer, i, :, width:] for i in range(sources)]
    best = functools.reduce(jnp.maximum, stats)
    weights = [jnp.exp(st - best) for st in stats]
    denom = sum(w * pltpu.roll(st, LANES - HEADS, 1) for w, st in zip(weights, stats))
    out = jnp.zeros((rows, width), F32)
    for i in range(sources):
        c = weights[i] / denom
        full = jnp.zeros((rows, width), F32)
        for h in range(HEADS):
            full = jnp.where(masks[h], c[:, h : h + 1], full)
        out = out + full * got[layer, i, :, :width]
    return out


def far_first(me, k, n):
    up = k + jnp.where(k >= me, 1, 0)
    down = n - 1 - k - jnp.where(n - 1 - k <= me, 1, 0)
    return jnp.where(me < n // 2, down, up)


def kernel(na, nb, *refs):
    (fa, fb), weights, (out_a, out_b) = refs[:2], refs[2:14], refs[14:16]
    (xa, xb, sa, sb, ga, gb), rest = refs[16:22], refs[22:]
    held, rest = rest[:12], rest[12:]
    his, los = rest[:5], rest[5:10]
    load, vec, in_sem, xs, xr, ys, yr, ps, pr, qs, qr = rest[10:]
    wqk, bqk, wv, bv, wo, bo, wh, bh, gain, nbias, wf, bf = held
    layers, _, ra, width = xa.shape
    rb = xb.shape[2]
    scale = (width // HEADS) ** (-0.5)
    ma, mb = lax.axis_index("ba"), lax.axis_index("aa")

    first = [
        pltpu.make_async_copy(fa, xa.at[0, ma], in_sem.at[0]),
        pltpu.make_async_copy(fb, xb.at[0, mb], in_sem.at[1]),
    ]
    for c in first:
        c.start()
    small = [(w, h) for w, h in zip(weights, held) if len(w.shape) == 2]
    large = [(w, h) for w, h in zip(weights, held) if len(w.shape) == 3]
    vectors = [pltpu.make_async_copy(w, h, vec.at[i]) for i, (w, h) in enumerate(small)]
    loads = [
        [pltpu.make_async_copy(w.at[j], h.at[j], load.at[j, i]) for i, (w, h) in enumerate(large)]
        for j in range(layers)
    ]
    for c in loads[0][:2] + vectors + loads[0][2:]:
        c.start()
    for later in loads[1:]:
        for c in later:
            c.start()

    barrier = pltpu.get_barrier_semaphore()
    for axis, me, n in (("ba", ma, nb), ("aa", mb, na)):
        for d in range(1, n):
            pl.semaphore_signal(
                barrier,
                inc=1,
                device_id={axis: (me + d) % n},
                device_id_type=pl.DeviceIdType.MESH,
            )
    pl.semaphore_wait(barrier, na + nb - 2)
    for c in first:
        c.wait()

    sent = []

    def exchange(axis, me, n, source, target, layer, ssem, rsem):
        arrive = []
        for d in range(1, n):
            peer = far_first(me, d - 1, n) if axis == "aa" else (me + d) % n
            copy = pltpu.make_async_remote_copy(
                src_ref=source(peer),
                dst_ref=target.at[layer, me],
                send_sem=ssem.at[layer, d],
                recv_sem=rsem.at[layer, me],
                device_id={axis: peer},
                device_id_type=pl.DeviceIdType.MESH,
            )
            copy.start()
            sent.append(copy)
            arrive.append(
                pltpu.make_async_remote_copy(
                    src_ref=target.at[layer, peer],
                    dst_ref=target.at[layer, peer],
                    send_sem=ssem.at[layer, d],
                    recv_sem=rsem.at[layer, peer],
                    device_id={axis: peer},
                    device_id_type=pl.DeviceIdType.MESH,
                )
            )
        return arrive

    matrices = (wqk, wv, wo, wh, wf)

    def narrow(which, layer):
        for i in which:
            loads[layer][i].wait()
            his[i][layer], los[i][layer] = split(matrices[i][layer])

    def wide(i, layer):
        return his[i][layer], los[i][layer]

    for l in range(layers):
        far = exchange("aa", mb, na, lambda p: xb.at[l, mb], xb, l, ys, yr)
        near = exchange("ba", ma, nb, lambda p: xa.at[l, ma], xa, l, xs, xr)
        if l == 0:
            narrow(range(2), 0)
            for c in vectors:
                c.wait()
        for c in near:
            c.wait_recv()
        rows_a = split(xa[l].reshape(nb * ra, width))
        w, u = wide(0, l), wide(1, l)
        qa = split(dot3(rows_a, w) + bqk[l : l + 1])
        va = split(dot3(rows_a, u) + bv[l : l + 1])
        for c in far:
            c.wait_recv()
        rows_b = split(xb[l].reshape(na * rb, width))
        qb = split(dot3(rows_b, w) + bqk[l : l + 1])
        vb = split(dot3(rows_b, u) + bv[l : l + 1])

        numer, stats = attend(qb, qa, va, scale)
        sb[l, :, :, :width] = numer.reshape(na, rb, width)
        sb[l, :, :, width:] = stats.reshape(na, rb, LANES)
        arrive = exchange("aa", mb, na, lambda p: sb.at[l, p], gb, l, qs, qr)
        numer, stats = attend(qa, qb, vb, scale)
        sa[l, :, :, :width] = numer.reshape(nb, ra, width)
        sa[l, :, :, width:] = stats.reshape(nb, ra, LANES)
        arrive += exchange("ba", ma, nb, lambda p: sa.at[l, p], ga, l, ps, pr)
        ga[l, ma] = sa[l, ma]
        gb[l, mb] = sb[l, mb]
        if l == 0:
            narrow(range(2, 5), 0)
            for j in range(1, layers):
                narrow(range(5), j)
        for c in arrive:
            c.wait_recv()

        x = jnp.concatenate([xa[l, ma], xb[l, mb]], 0)
        msg = jnp.concatenate([settle(ga, l), settle(gb, l)], 0)
        y = dot3(split(msg), wide(2, l)) + bo[l : l + 1]
        joined = split(jnp.concatenate([x, y], 1))
        hidden = dot3(joined, wide(3, l)) + bh[l : l + 1]
        centred = hidden - jnp.mean(hidden, 1, keepdims=True)
        spread = jnp.mean(centred * centred, 1, keepdims=True)
        normed = centred / jnp.sqrt(spread + 1e-05) * gain[l : l + 1] + nbias[l : l + 1]
        active = 0.5 * normed * (1.0 + erf(normed * (0.5**0.5)))
        x = x + dot3(split(active), wide(4, l)) + bf[l : l + 1]
        if l + 1 < layers:
            xa[l + 1, ma] = x[:ra]
            xb[l + 1, mb] = x[ra:]
        else:
            out_a[...] = x[:ra]
            out_b[...] = x[ra:]
    for c in sent:
        c.wait_send()


def shards(na, nb, *args):
    fa, fb, *weights = args
    layers = weights[0].shape[0]
    (ra, width), rb = fa.shape, fb.shape[0]
    packed = width + LANES
    matrices = [weights[i] for i in (0, 2, 4, 6, 10)]
    dma = pltpu.SemaphoreType.DMA
    scratch = [
        pltpu.VMEM((layers, nb, ra, width), F32),
        pltpu.VMEM((layers, na, rb, width), F32),
        pltpu.VMEM((layers, nb, ra, packed), F32),
        pltpu.VMEM((layers, na, rb, packed), F32),
        pltpu.VMEM((layers, nb, ra, packed), F32),
        pltpu.VMEM((layers, na, rb, packed), F32),
    ]
    scratch += [pltpu.VMEM(w.shape, F32) for w in weights]
    scratch += [pltpu.VMEM(w.shape, BF16) for w in matrices] * 2
    scratch += [dma((layers, len(matrices))), dma((len(weights) - len(matrices),)), dma((2,))]
    scratch += [dma((layers, n)) for n in (nb, nb, na, na, nb, nb, na, na)]
    any_spec = pl.BlockSpec(memory_space=pltpu.HBM)
    vmem = pl.BlockSpec(memory_space=pltpu.VMEM)
    return tuple(
        pl.pallas_call(
            functools.partial(kernel, na, nb),
            out_shape=(
                pltpu.VMEM(fa.shape, F32),
                pltpu.VMEM(fb.shape, F32),
            ),
            in_specs=[any_spec] * len(args),
            out_specs=(vmem, vmem),
            scratch_shapes=scratch,
            compiler_params=pltpu.CompilerParams(
                collective_id=0, has_side_effects=True, vmem_limit_bytes=60 * 1024 * 1024
            ),
        )(*args)
    )


def solution(mesh):
    in_specs = (P(("pairs", "aa", "ba"), None), P(("pairs", "ba", "aa"), None)) + (P(),) * 12
    out_specs = (P(("pairs", "aa", "ba"), None), P(("pairs", "ba", "aa"), None))
    return jax.shard_map(
        functools.partial(shards, mesh.shape["aa"], mesh.shape["ba"]),
        mesh=mesh,
        in_specs=in_specs,
        out_specs=out_specs,
        check_vma=False,
    )
```
